32 devices in a mesh: gx: 8 (over z, y), gy: 4 (over x, core).
Axes of the slice: x: 2, y: 2, z: 4, core: 2. Of those that a mesh axis runs over, the one named last changes fastest.
Arguments:
- goal_embed: bfloat16 [4096, 128], P(('gx', 'gy')), may hold values from -6 to 6
- goal_bins: int32 [4096], P(('gx', 'gy')), may hold values from 0 to 2047, as said below
- goal_weights: float32 [4096], P(('gx', 'gy')), may hold values from 0.1 to 10
Outputs:
- bin_mean: float32 [2048, 128], P(('gx', 'gy'))
- rarity: float32 [2048], P(('gx', 'gy'))
The draws below stay inside these ranges and needn't reach their ends.
Inputs may be any that keep to these rules, and one draw needn't show every extreme that they name: `goal_bins`: bin b belongs to owner b // 64, owners numbered in the order of gx then gy. Of the goals of one device, at most 8 fall in the bins of one owner; some owner receives exactly 8 goals from every device.
All inputs are finite; a program needn't handle non-finite values.
Results may differ from the reference program's by a relative error of at most 0.0029.
Values may be sent and summed in bfloat16 or wider, within the bound.
A program may use at most 64 MiB of HBM per device.

```python
import math
import jax
import jax.numpy as jnp

E = 128
BINS_DEV = 64
G_DEV = 128
GOALS = 4096
BINS = 2048
N_GX = 8
N_GY = 4


def draw_goal_bins(key, part):
    devices = N_GX * N_GY
    capacity = max(2, 2 * G_DEV // devices)
    key_common = jax.random.fold_in(key, 11)
    key_blocks = jax.random.fold_in(key, 12)
    key_offset = jax.random.fold_in(key, 13)
    common = jax.random.randint(key_common, (), 0, devices).astype(jnp.int32)

    def one_block(block_key):
        key_slots = jax.random.fold_in(block_key, 1)
        key_order = jax.random.fold_in(block_key, 2)
        slots = jax.random.permutation(key_slots, (devices - 1) * capacity).astype(jnp.int32)
        others = slots[:G_DEV - capacity] // capacity
        others = others + (others >= common).astype(jnp.int32)
        owners = jnp.concatenate([jnp.zeros((capacity,), jnp.int32) + common, others.astype(jnp.int32)])
        return jax.random.permutation(key_order, owners).astype(jnp.int32)
    owners = jax.vmap(one_block)(jax.random.split(key_blocks, devices)).reshape(-1)
    offsets = jax.random.randint(key_offset, (G_DEV * devices,), 0, BINS_DEV).astype(jnp.int32)
    return (owners * BINS_DEV + offsets).astype(jnp.int32)


def steps_of(rng, extent, pieces, least, high):
    gain = 1.0
    for position, shards_of in pieces:
        draws = jax.random.uniform(jax.random.fold_in(jax.random.fold_in(rng, 6), position), (shards_of,), jnp.float32, least / len(pieces), high / len(pieces))
        gain = gain * jnp.repeat(jnp.exp(draws), extent[position] // shards_of).reshape((-1,) + (1,) * (len(extent) - 1 - position))
    return gain


def gaussian(stream_key, dims, spread, reach, cuts=(), kind=jnp.bfloat16):
    array = jax.random.normal(stream_key, dims, jnp.float32) * spread
    if len(cuts) > 0:
        array = steps_of(stream_key, dims, cuts, -0.22, 0.18) * array
    return jnp.clip(array, min=-reach, max=reach).astype(kind)


def setup_inputs(seed: int = 0) -> dict:
    streams_of = jax.random.split(jax.random.key(seed), 4)
    goal_embed = gaussian(streams_of[0], (GOALS, E), 1.0, 6.0, ((0, 32),))
    goal_bins = draw_goal_bins(jax.random.fold_in(streams_of[3], 71), 0)
    goal_weights = jnp.clip(jnp.exp(math.log(10.0) - 4.6051702 * jax.random.uniform(streams_of[2], (GOALS,), jnp.float32) ** steps_of(streams_of[2], (GOALS,), ((0, 32),), -0.2, 0.2)), 0.1, 10.0)
    return {"goal_embed": goal_embed, "goal_bins": goal_bins, "goal_weights": goal_weights}


def reference(goal_embed, goal_bins, goal_weights):
    scaled = (goal_weights[:, None] * goal_embed.astype(jnp.float32)).astype(jnp.bfloat16)
    bin_sums = jax.ops.segment_sum(scaled.astype(jnp.float32), goal_bins, num_segments=BINS)
    bin_mass = jax.ops.segment_sum(goal_weights, goal_bins, num_segments=BINS)
    total_mass = jnp.sum(goal_weights)
    bin_mean = bin_sums / (bin_mass[:, None] + 1.0)
    rarity = jnp.log(total_mass / BINS) - jnp.log(bin_mass + 1.0)
    return bin_mean, rarity
```

```python
import functools

import jax
import jax.numpy as jnp
from jax import lax
from jax.experimental import pallas as pl
from jax.experimental.pallas import tpu as pltpu
from jax.sharding import PartitionSpec as P

BINS_DEV = 64
MESH = pl.DeviceIdType.MESH


def each(count, body):
    if count <= 64:
        for k in range(count):
            body(k)
    else:
        lax.fori_loop(0, count, lambda k, c: (body(k), c)[1], 0)


def split3(x):
    hi = x.astype(jnp.bfloat16).astype(jnp.float32)
    rest = x - hi
    mid = rest.astype(jnp.bfloat16).astype(jnp.float32)
    return hi, mid, rest - mid


def kernel(across, along, stride, embed_ref, bins_ref, weights_ref, mean_ref, rarity_ref, send, recv, send_sem, recv_sem):
    n = across * along
    goals, width = embed_ref.shape
    me = lax.axis_index("gx") * along + lax.axis_index("gy")

    def device(k):
        d = lax.rem(me + k + 1, n)
        return {"gx": d // along, "gy": lax.rem(d, along)}

    barrier = pltpu.get_barrier_semaphore()
    each(n - 1, lambda k: pl.semaphore_signal(barrier, inc=1, device_id=device(k), device_id_type=MESH))

    bins_row = jnp.broadcast_to(bins_ref[...], (goals, goals))
    weights_row = jnp.broadcast_to(weights_ref[...], (goals, goals))
    bins_col = bins_row.T
    weights_col = weights_row.T
    shift = BINS_DEV.bit_length() - 1
    owners_row = lax.shift_right_logical(bins_row, shift)
    owners_col = lax.shift_right_logical(bins_col, shift)
    sub = lax.broadcasted_iota(jnp.int32, (goals, goals), 0)
    lane = lax.broadcasted_iota(jnp.int32, (goals, goals), 1)
    earlier = (owners_row == owners_col) & (sub < lane)
    place = jnp.sum(earlier.astype(jnp.float32), axis=0, keepdims=True).astype(jnp.int32)
    ahead = owners_row[:1] - me - 1
    ahead = jnp.where(ahead < 0, ahead + n, ahead)
    slot = ahead * stride + place
    rows_iota = lax.broadcasted_iota(jnp.int32, (n * stride, goals), 0)
    pick = (rows_iota == slot).astype(jnp.bfloat16)

    scaled = (weights_col[:, :width] * embed_ref[...].astype(jnp.float32)).astype(jnp.bfloat16)
    hi, mid, lo = split3(weights_col)
    offset = bins_col - owners_col * BINS_DEV
    tags = (lane == offset).astype(jnp.float32)
    for i, part in enumerate((hi, mid, lo)):
        tags = jnp.where(lane == BINS_DEV + i, part, tags)
    rows = jnp.dot(pick, scaled, preferred_element_type=jnp.float32)
    marks = jnp.dot(pick, tags.astype(jnp.bfloat16), preferred_element_type=jnp.float32)

    local = jnp.sum(weights_ref[...], axis=1, keepdims=True)
    t_hi, t_mid, t_lo = split3(local)
    lanes = lax.broadcasted_iota(jnp.int32, (1, 1, goals), 2)
    first = lax.broadcasted_iota(jnp.int32, (1, stride, goals), 1) == 0
    extra = jnp.zeros((1, stride, goals), jnp.float32)
    for i, part in enumerate((t_hi, t_mid, t_lo, jnp.ones_like(local))):
        extra = jnp.where(first & (lanes == BINS_DEV + 3 + i), part[None], extra)
    rows = rows.reshape(n, stride, width).astype(jnp.bfloat16)
    marks = (marks.reshape(n, stride, goals) + extra).astype(jnp.bfloat16)
    send[:, :, :width] = rows[: n - 1]
    send[:, :, width:] = marks[: n - 1]
    recv[n - 1, :, :width] = rows[n - 1]
    recv[n - 1, :, width:] = marks[n - 1]

    pl.semaphore_wait(barrier, n - 1)

    def start(k):
        pltpu.make_async_remote_copy(
            src_ref=send.at[k],
            dst_ref=recv.at[k],
            send_sem=send_sem,
            recv_sem=recv_sem,
            device_id=device(k),
            device_id_type=MESH,
        ).start()

    each(n - 1, start)
    landed = recv.at[pl.ds(0, n - 1)]
    pltpu.make_async_copy(landed, landed, recv_sem).wait()

    data = recv[...].astype(jnp.float32).reshape(n * stride, width + goals).astype(jnp.bfloat16)
    marks = data[:, width:]
    sums = lax.dot_general(marks, data, (((0,), (0,)), ((), ())), preferred_element_type=jnp.float32)
    gram = sums[:, width:]
    g_lane = lax.broadcasted_iota(jnp.int32, (goals, goals), 1)
    g_sub = lax.broadcasted_iota(jnp.int32, (goals, goals), 0)
    is_w_lane = (g_lane >= BINS_DEV) & (g_lane < BINS_DEV + 3)
    is_w_sub = (g_sub >= BINS_DEV) & (g_sub < BINS_DEV + 3)
    mass_col = jnp.sum(jnp.where(is_w_lane, gram, 0.0), axis=1, keepdims=True)[:BINS_DEV]
    mass_row = jnp.sum(jnp.where(is_w_sub, gram, 0.0), axis=0, keepdims=True)[:, :BINS_DEV]
    total = jnp.sum(
        jnp.where((g_lane >= BINS_DEV + 3) & (g_lane < BINS_DEV + 6), gram, 0.0)[BINS_DEV + 6 : BINS_DEV + 7],
        axis=1,
        keepdims=True,
    )
    mean_ref[...] = sums[:BINS_DEV, :width] / (mass_col + 1.0)
    rarity_ref[...] = jnp.log(total / (BINS_DEV * n)) - jnp.log(mass_row + 1.0)
    pltpu.make_async_copy(send, send, send_sem).wait()


def shards(goal_embed, goal_bins, goal_weights):
    goals, width = goal_embed.shape
    across = lax.axis_size("gx")
    along = lax.axis_size("gy")
    n = across * along
    capacity = max(2, 2 * goals // n)
    stride = -(-capacity // 8) * 8
    mean, rarity = pl.pallas_call(
        functools.partial(kernel, across, along, stride),
        out_shape=(
            jax.ShapeDtypeStruct((BINS_DEV, width), jnp.float32),
            jax.ShapeDtypeStruct((1, BINS_DEV), jnp.float32),
        ),
        in_specs=[pl.BlockSpec(memory_space=pltpu.VMEM)] * 3,
        out_specs=(pl.BlockSpec(memory_space=pltpu.VMEM),) * 2,
        scratch_shapes=[
            pltpu.VMEM((n - 1, stride, width + goals), jnp.bfloat16),
            pltpu.VMEM((n, stride, width + goals), jnp.bfloat16),
            pltpu.SemaphoreType.DMA,
            pltpu.SemaphoreType.DMA,
        ],
        compiler_params=pltpu.CompilerParams(collective_id=0, has_side_effects=True),
    )(goal_embed, goal_bins.reshape(1, goals), goal_weights.reshape(1, goals))
    return mean, rarity.reshape(BINS_DEV)


def solution(mesh):
    in_specs = (P(("gx", "gy"), None), P(("gx", "gy")), P(("gx", "gy")))
    out_specs = (P(("gx", "gy"), None), P(("gx", "gy")))
    return jax.shard_map(shards, mesh=mesh, in_specs=in_specs, out_specs=out_specs, check_vma=False)
```

```python
import functools

import jax
import jax.numpy as jnp
from jax import lax
from jax.experimental import pallas as pl
from jax.experimental.pallas import tpu as pltpu
from jax.sharding import PartitionSpec as P

BINS_DEV = 64
MESH = pl.DeviceIdType.MESH


def each(count, body):
    if count <= 64:
        for k in range(count):
            body(k)
    else:
        lax.fori_loop(0, count, lambda k, c: (body(k), c)[1], 0)


def split3(x):
    hi = x.astype(jnp.bfloat16).astype(jnp.float32)
    rest = x - hi
    mid = rest.astype(jnp.bfloat16).astype(jnp.float32)
    return hi, mid, rest - mid


def kernel(across, along, stride, embed_hbm, bins_hbm, weights_hbm, mean_ref, rarity_ref, send, recv, send_sem, recv_sem, embed_ref, bins_ref, weights_ref, in_sem):
    loads = [pltpu.make_async_copy(a, b, in_sem.at[i]) for i, (a, b) in enumerate(((bins_hbm, bins_ref), (weights_hbm, weights_ref), (embed_hbm, embed_ref)))]
    for c in loads:
        c.start()
    n = across * along
    goals, width = embed_ref.shape
    me = lax.axis_index("gx") * along + lax.axis_index("gy")

    def device(k):
        d = lax.rem(me + k + 1, n)
        return {"gx": d // along, "gy": lax.rem(d, along)}

    barrier = pltpu.get_barrier_semaphore()
    each(n - 1, lambda k: pl.semaphore_signal(barrier, inc=1, device_id=device(k), device_id_type=MESH))

    for c in loads:
        c.wait()
    bins_row = jnp.broadcast_to(bins_ref[...], (goals, goals))
    weights_row = jnp.broadcast_to(weights_ref[...], (goals, goals))
    bins_col = bins_row.T
    weights_col = weights_row.T
    shift = BINS_DEV.bit_length() - 1
    owners_row = lax.shift_right_logical(bins_row, shift)
    owners_col = lax.shift_right_logical(bins_col, shift)
    sub = lax.broadcasted_iota(jnp.int32, (goals, goals), 0)
    lane = lax.broadcasted_iota(jnp.int32, (goals, goals), 1)
    earlier = (owners_row == owners_col) & (sub < lane)
    place = jnp.sum(earlier.astype(jnp.float32), axis=0, keepdims=True).astype(jnp.int32)
    ahead = owners_row[:1] - me - 1
    ahead = jnp.where(ahead < 0, ahead + n, ahead)
    slot = ahead * stride + place
    rows_iota = lax.broadcasted_iota(jnp.int32, (n * stride, goals), 0)
    pick = (rows_iota == slot).astype(jnp.bfloat16)

    scaled = (weights_col[:, :width] * embed_ref[...].astype(jnp.float32)).astype(jnp.bfloat16)
    hi, mid, lo = split3(weights_col)
    offset = bins_col - owners_col * BINS_DEV
    tags = (lane == offset).astype(jnp.float32)
    for i, part in enumerate((hi, mid, lo)):
        tags = jnp.where(lane == BINS_DEV + i, part, tags)
    rows = jnp.dot(pick, scaled, preferred_element_type=jnp.float32)
    marks = jnp.dot(pick, tags.astype(jnp.bfloat16), preferred_element_type=jnp.float32)

    local = jnp.sum(weights_ref[...], axis=1, keepdims=True)
    t_hi, t_mid, t_lo = split3(local)
    lanes = lax.broadcasted_iota(jnp.int32, (1, 1, goals), 2)
    first = lax.broadcasted_iota(jnp.int32, (1, stride, goals), 1) == 0
    extra = jnp.zeros((1, stride, goals), jnp.float32)
    for i, part in enumerate((t_hi, t_mid, t_lo, jnp.ones_like(local))):
        extra = jnp.where(first & (lanes == BINS_DEV + 3 + i), part[None], extra)
    rows = rows.reshape(n, stride, width).astype(jnp.bfloat16)
    marks = (marks.reshape(n, stride, goals) + extra).astype(jnp.bfloat16)
    send[:, :, :width] = rows[: n - 1]
    send[:, :, width:] = marks[: n - 1]
    recv[n - 1, :, :width] = rows[n - 1]
    recv[n - 1, :, width:] = marks[n - 1]

    pl.semaphore_wait(barrier, n - 1)

    def start(k):
        pltpu.make_async_remote_copy(
            src_ref=send.at[k],
            dst_ref=recv.at[k],
            send_sem=send_sem,
            recv_sem=recv_sem,
            device_id=device(k),
            device_id_type=MESH,
        ).start()

    each(n - 1, start)
    landed = recv.at[pl.ds(0, n - 1)]
    pltpu.make_async_copy(landed, landed, recv_sem).wait()

    data = recv[...].astype(jnp.float32).reshape(n * stride, width + goals).astype(jnp.bfloat16)
    marks = data[:, width:]
    sums = lax.dot_general(marks, data, (((0,), (0,)), ((), ())), preferred_element_type=jnp.float32)
    gram = sums[:, width:]
    g_lane = lax.broadcasted_iota(jnp.int32, (goals, goals), 1)
    g_sub = lax.broadcasted_iota(jnp.int32, (goals, goals), 0)
    is_w_lane = (g_lane >= BINS_DEV) & (g_lane < BINS_DEV + 3)
    is_w_sub = (g_sub >= BINS_DEV) & (g_sub < BINS_DEV + 3)
    mass_col = jnp.sum(jnp.where(is_w_lane, gram, 0.0), axis=1, keepdims=True)[:BINS_DEV]
    mass_row = jnp.sum(jnp.where(is_w_sub, gram, 0.0), axis=0, keepdims=True)[:, :BINS_DEV]
    total = jnp.sum(
        jnp.where((g_lane >= BINS_DEV + 3) & (g_lane < BINS_DEV + 6), gram, 0.0)[BINS_DEV + 6 : BINS_DEV + 7],
        axis=1,
        keepdims=True,
    )
    mean_ref[...] = sums[:BINS_DEV, :width] / (mass_col + 1.0)
    rarity_ref[...] = jnp.log(total / (BINS_DEV * n)) - jnp.log(mass_row + 1.0)
    pltpu.make_async_copy(send, send, send_sem).wait()


def put(mean, rarity, mean_hbm, rarity_hbm, sem):
    copies = [pltpu.make_async_copy(mean, mean_hbm, sem.at[0]), pltpu.make_async_copy(rarity, rarity_hbm, sem.at[1])]
    for c in copies:
        c.start()
    for c in copies:
        c.wait()


def shards(goal_embed, goal_bins, goal_weights):
    goals, width = goal_embed.shape
    across = lax.axis_size("gx")
    along = lax.axis_size("gy")
    n = across * along
    capacity = max(2, 2 * goals // n)
    stride = -(-capacity // 8) * 8
    mean, rarity = pl.pallas_call(
        functools.partial(kernel, across, along, stride),
        out_shape=(
            pltpu.VMEM((BINS_DEV, width), jnp.float32),
            pltpu.VMEM((1, BINS_DEV), jnp.float32),
        ),
        in_specs=[pl.BlockSpec(memory_space=pl.ANY)] * 3,
        out_specs=(pl.BlockSpec(memory_space=pltpu.VMEM),) * 2,
        scratch_shapes=[
            pltpu.VMEM((n - 1, stride, width + goals), jnp.bfloat16),
            pltpu.VMEM((n, stride, width + goals), jnp.bfloat16),
            pltpu.SemaphoreType.DMA,
            pltpu.SemaphoreType.DMA,
            pltpu.VMEM((goals, width), jnp.bfloat16),
            pltpu.VMEM((1, goals), jnp.int32),
            pltpu.VMEM((1, goals), jnp.float32),
            pltpu.SemaphoreType.DMA((3,)),
        ],
        compiler_params=pltpu.CompilerParams(collective_id=0, has_side_effects=True),
    )(goal_embed, goal_bins.reshape(1, goals), goal_weights.reshape(1, goals))
    mean, rarity = pl.pallas_call(
        put,
        out_shape=(
            jax.ShapeDtypeStruct((BINS_DEV, width), jnp.float32),
            jax.ShapeDtypeStruct((1, BINS_DEV), jnp.float32),
        ),
        in_specs=[pl.BlockSpec(memory_space=pltpu.VMEM)] * 2,
        out_specs=(pl.BlockSpec(memory_space=pl.ANY),) * 2,
        scratch_shapes=[pltpu.SemaphoreType.DMA((2,))],
    )(pltpu.with_memory_space_constraint(mean, pltpu.VMEM), pltpu.with_memory_space_constraint(rarity, pltpu.VMEM))
    return mean, rarity.reshape(BINS_DEV)


def solution(mesh):
    in_specs = (P(("gx", "gy"), None), P(("gx", "gy")), P(("gx", "gy")))
    out_specs = (P(("gx", "gy"), None), P(("gx", "gy")))
    return jax.shard_map(shards, mesh=mesh, in_specs=in_specs, out_specs=out_specs, check_vma=False)
```

```python
import functools

import jax
import jax.numpy as jnp
from jax import lax
from jax.experimental import pallas as pl
from jax.experimental.pallas import tpu as pltpu
from jax.sharding import PartitionSpec as P

BINS_DEV = 64
MESH = pl.DeviceIdType.MESH


def each(count, body):
    if count <= 64:
        for k in range(count):
            body(k)
    else:
        lax.fori_loop(0, count, lambda k, c: (body(k), c)[1], 0)


def split3(x):
    hi = x.astype(jnp.bfloat16).astype(jnp.float32)
    rest = x - hi
    mid = rest.astype(jnp.bfloat16).astype(jnp.float32)
    return hi, mid, rest - mid


def kernel(across, along, stride, embed_hbm, bins_hbm, weights_hbm, mean_ref, rarity_ref, send, recv, send_sem, recv_sem, embed_ref, bins_ref, weights_ref, in_sem):
    loads = [pltpu.make_async_copy(a, b, in_sem.at[i]) for i, (a, b) in enumerate(((bins_hbm, bins_ref), (weights_hbm, weights_ref), (embed_hbm, embed_ref)))]
    for c in loads:
        c.start()
    n = across * along
    goals, width = embed_ref.shape
    me = lax.axis_index("gx") * along + lax.axis_index("gy")

    def device(k):
        d = lax.rem(me + k + 1, n)
        return {"gx": d // along, "gy": lax.rem(d, along)}

    barrier = pltpu.get_barrier_semaphore()
    each(n - 1, lambda k: pl.semaphore_signal(barrier, inc=1, device_id=device(k), device_id_type=MESH))

    for c in loads:
        c.wait()
    bins_row = jnp.broadcast_to(bins_ref[...], (goals, goals))
    weights_row = jnp.broadcast_to(weights_ref[...], (goals, goals))
    bins_col = bins_row.T
    weights_col = weights_row.T
    shift = BINS_DEV.bit_length() - 1
    owners_row = lax.shift_right_logical(bins_row, shift)
    owners_col = lax.shift_right_logical(bins_col, shift)
    sub = lax.broadcasted_iota(jnp.int32, (goals, goals), 0)
    lane = lax.broadcasted_iota(jnp.int32, (goals, goals), 1)
    earlier = (owners_row == owners_col) & (sub < lane)
    place = jnp.sum(earlier.astype(jnp.float32), axis=0, keepdims=True).astype(jnp.int32)
    ahead = owners_row[:1] - me - 1
    ahead = jnp.where(ahead < 0, ahead + n, ahead)
    rows_iota = lax.broadcasted_iota(jnp.int32, (n * stride, goals), 0)
    base = ahead * stride
    pick = (rows_iota == base + place).astype(jnp.bfloat16)
    group = ((rows_iota >= base) & (rows_iota < base + stride)).astype(jnp.bfloat16)

    offset = bins_col - owners_col * BINS_DEV
    place_col = jnp.sum(((owners_row == owners_col) & (lane < sub)).astype(jnp.float32), axis=1, keepdims=True)
    hit = (lane == offset) | (lane == offset + BINS_DEV)
    masses = jnp.zeros((n * stride, goals), jnp.float32)
    for part in split3(weights_col):
        spread = jnp.where(hit, part, 0.0).astype(jnp.bfloat16)
        masses = masses + jnp.dot(group, spread, preferred_element_type=jnp.float32)
    spot = jnp.where(lane == place_col.astype(jnp.int32) + BINS_DEV, offset.astype(jnp.float32), 0.0)
    offsets = jnp.dot(group, spot.astype(jnp.bfloat16), preferred_element_type=jnp.float32)
    local = jnp.sum(weights_ref[...], axis=1, keepdims=True)
    t_lane = lax.broadcasted_iota(jnp.int32, (1, goals), 1)
    extra = jnp.zeros((1, goals), jnp.float32)
    for i, part in enumerate(split3(local)):
        extra = jnp.where(t_lane == BINS_DEV + stride + i, part, extra)
    hi, mid, lo = split3(masses)
    low_half = lax.broadcasted_iota(jnp.int32, (n * stride, goals), 1) < BINS_DEV
    line = lax.rem(rows_iota, stride)
    marks = jnp.where(line == 0, jnp.where(low_half, lo, offsets + extra), jnp.where(low_half, hi, mid))
    scaled = (weights_col[:, :width] * embed_ref[...].astype(jnp.float32)).astype(jnp.bfloat16)
    rows = jnp.dot(pick, scaled, preferred_element_type=jnp.float32)
    full = jnp.concatenate([rows.reshape(n, stride, width), marks.reshape(n, stride, goals)], axis=1)
    full = full.astype(jnp.bfloat16)
    send[...] = full[: n - 1]
    recv[n - 1] = full[n - 1]

    pl.semaphore_wait(barrier, n - 1)

    def start(k):
        pltpu.make_async_remote_copy(
            src_ref=send.at[k, pl.ds(0, stride + 2)],
            dst_ref=recv.at[k, pl.ds(0, stride + 2)],
            send_sem=send_sem,
            recv_sem=recv_sem,
            device_id=device(k),
            device_id_type=MESH,
        ).start()

    each(n - 1, start)
    landed = recv.at[pl.ds(0, n - 1), pl.ds(0, stride + 2)]
    pltpu.make_async_copy(landed, landed, recv_sem).wait()

    data = recv[...].astype(jnp.float32)
    tags = data[:, stride:]
    s_sub = lax.broadcasted_iota(jnp.int32, (n, stride, goals), 1)
    s_lane = lax.broadcasted_iota(jnp.int32, (n, stride, goals), 2)
    spread = jnp.where(s_lane == s_sub + BINS_DEV, jnp.broadcast_to(tags[:, :1], (n, stride, goals)), 0.0)
    labels = jnp.sum(spread, axis=2, keepdims=True).astype(jnp.int32)
    choose = (s_lane == labels).astype(jnp.float32).reshape(n * stride, goals).astype(jnp.bfloat16)
    values = data[:, :stride].reshape(n * stride, width).astype(jnp.bfloat16)
    sums = lax.dot_general(choose, values, (((0,), (0,)), ((), ())), preferred_element_type=jnp.float32)
    added = jnp.sum(tags, axis=0)
    low, high = added[:1], added[1:2]
    mass = high + pltpu.roll(high, goals - BINS_DEV, 1) + low
    total = jnp.sum(
        jnp.where((t_lane >= BINS_DEV + stride) & (t_lane < BINS_DEV + stride + 3), low, 0.0), axis=1, keepdims=True
    )
    mass_col = jnp.broadcast_to(mass, (goals, goals)).T
    mean_ref[...] = sums[:BINS_DEV] / (mass_col[:BINS_DEV, :width] + 1.0)
    rarity_ref[...] = jnp.log(total / (BINS_DEV * n)) - jnp.log(mass[:, :BINS_DEV] + 1.0)
    sent = send.at[:, pl.ds(0, stride + 2)]
    pltpu.make_async_copy(sent, sent, send_sem).wait()


def put(mean, rarity, mean_hbm, rarity_hbm, sem):
    copies = [pltpu.make_async_copy(mean, mean_hbm, sem.at[0]), pltpu.make_async_copy(rarity, rarity_hbm, sem.at[1])]
    for c in copies:
        c.start()
    for c in copies:
        c.wait()


def shards(goal_embed, goal_bins, goal_weights):
    goals, width = goal_embed.shape
    across = lax.axis_size("gx")
    along = lax.axis_size("gy")
    n = across * along
    capacity = max(2, 2 * goals // n)
    stride = -(-capacity // 8) * 8
    mean, rarity = pl.pallas_call(
        functools.partial(kernel, across, along, stride),
        out_shape=(
            pltpu.VMEM((BINS_DEV, width), jnp.float32),
            pltpu.VMEM((1, BINS_DEV), jnp.float32),
        ),
        in_specs=[pl.BlockSpec(memory_space=pl.ANY)] * 3,
        out_specs=(pl.BlockSpec(memory_space=pltpu.VMEM),) * 2,
        scratch_shapes=[
            pltpu.VMEM((n - 1, 2 * stride, width), jnp.bfloat16),
            pltpu.VMEM((n, 2 * stride, width), jnp.bfloat16),
            pltpu.SemaphoreType.DMA,
            pltpu.SemaphoreType.DMA,
            pltpu.VMEM((goals, width), jnp.bfloat16),
            pltpu.VMEM((1, goals), jnp.int32),
            pltpu.VMEM((1, goals), jnp.float32),
            pltpu.SemaphoreType.DMA((3,)),
        ],
        compiler_params=pltpu.CompilerParams(collective_id=0, has_side_effects=True),
    )(goal_embed, goal_bins.reshape(1, goals), goal_weights.reshape(1, goals))
    mean, rarity = pl.pallas_call(
        put,
        out_shape=(
            jax.ShapeDtypeStruct((BINS_DEV, width), jnp.float32),
            jax.ShapeDtypeStruct((1, BINS_DEV), jnp.float32),
        ),
        in_specs=[pl.BlockSpec(memory_space=pltpu.VMEM)] * 2,
        out_specs=(pl.BlockSpec(memory_space=pl.ANY),) * 2,
        scratch_shapes=[pltpu.SemaphoreType.DMA((2,))],
    )(pltpu.with_memory_space_constraint(mean, pltpu.VMEM), pltpu.with_memory_space_constraint(rarity, pltpu.VMEM))
    return mean, rarity.reshape(BINS_DEV)


def solution(mesh):
    in_specs = (P(("gx", "gy"), None), P(("gx", "gy")), P(("gx", "gy")))
    out_specs = (P(("gx", "gy"), None), P(("gx", "gy")))
    return jax.shard_map(shards, mesh=mesh, in_specs=in_specs, out_specs=out_specs, check_vma=False)
```

```python
import functools

import jax
import jax.numpy as jnp
from jax import lax
from jax.experimental import pallas as pl
from jax.experimental.pallas import tpu as pltpu
from jax.sharding import PartitionSpec as P

BINS_DEV = 64
MESH = pl.DeviceIdType.MESH


def each(count, body):
    if count <= 64:
        for k in range(count):
            body(k)
    else:
        lax.fori_loop(0, count, lambda k, c: (body(k), c)[1], 0)


def split3(x):
    hi = x.astype(jnp.bfloat16).astype(jnp.float32)
    rest = x - hi
    mid = rest.astype(jnp.bfloat16).astype(jnp.float32)
    return hi, mid, rest - mid


def kernel(across, along, stride, embed_hbm, bins_hbm, weights_hbm, mean_ref, rarity_ref, send, recv, send_sem, recv_sem, embed_ref, bins_ref, weights_ref, in_sem):
    loads = [pltpu.make_async_copy(a, b, in_sem.at[i]) for i, (a, b) in enumerate(((bins_hbm, bins_ref), (weights_hbm, weights_ref), (embed_hbm, embed_ref)))]
    for c in loads:
        c.start()
    n = across * along
    near = n // 4
    goals, width = embed_ref.shape
    me = lax.axis_index("gx") * along + lax.axis_index("gy")

    def device(k):
        d = lax.rem(me + k + 1, n)
        return {"gx": d // along, "gy": lax.rem(d, along)}

    barrier = pltpu.get_barrier_semaphore()
    each(n - 1, lambda k: pl.semaphore_signal(barrier, inc=1, device_id=device(k), device_id_type=MESH))

    for c in loads:
        c.wait()
    bins_row = jnp.broadcast_to(bins_ref[...], (goals, goals))
    weights_row = jnp.broadcast_to(weights_ref[...], (goals, goals))
    bins_col = bins_row.T
    weights_col = weights_row.T
    shift = BINS_DEV.bit_length() - 1
    owners_row = lax.shift_right_logical(bins_row, shift)
    owners_col = lax.shift_right_logical(bins_col, shift)
    sub = lax.broadcasted_iota(jnp.int32, (goals, goals), 0)
    lane = lax.broadcasted_iota(jnp.int32, (goals, goals), 1)
    earlier = (owners_row == owners_col) & (sub < lane)
    place = jnp.sum(earlier.astype(jnp.float32), axis=0, keepdims=True).astype(jnp.int32)
    ahead = owners_row[:1] - me - 1
    ahead = jnp.where(ahead < 0, ahead + n, ahead)
    rows_iota = lax.broadcasted_iota(jnp.int32, (n * stride, goals), 0)
    base = ahead * stride
    pick = (rows_iota == base + place).astype(jnp.bfloat16)
    group = ((rows_iota >= base) & (rows_iota < base + stride)).astype(jnp.bfloat16)

    offset = bins_col - owners_col * BINS_DEV
    place_col = jnp.sum(((owners_row == owners_col) & (lane < sub)).astype(jnp.float32), axis=1, keepdims=True)
    hit = (lane == offset) | (lane == offset + BINS_DEV)
    masses = jnp.zeros((n * stride, goals), jnp.float32)
    for part in split3(weights_col):
        spread = jnp.where(hit, part, 0.0).astype(jnp.bfloat16)
        masses = masses + jnp.dot(group, spread, preferred_element_type=jnp.float32)
    spot = jnp.where(lane == place_col.astype(jnp.int32) + BINS_DEV, offset.astype(jnp.float32), 0.0)
    offsets = jnp.dot(group, spot.astype(jnp.bfloat16), preferred_element_type=jnp.float32)
    local = jnp.sum(weights_ref[...], axis=1, keepdims=True)
    t_lane = lax.broadcasted_iota(jnp.int32, (1, goals), 1)
    extra = jnp.zeros((1, goals), jnp.float32)
    for i, part in enumerate(split3(local)):
        extra = jnp.where(t_lane == BINS_DEV + stride + i, part, extra)
    hi, mid, lo = split3(masses)
    low_half = lax.broadcasted_iota(jnp.int32, (n * stride, goals), 1) < BINS_DEV
    line = lax.rem(rows_iota, stride)
    marks = jnp.where(line == 0, jnp.where(low_half, lo, offsets + extra), jnp.where(low_half, hi, mid))
    scaled = (weights_col[:, :width] * embed_ref[...].astype(jnp.float32)).astype(jnp.bfloat16)
    rows = jnp.dot(pick, scaled, preferred_element_type=jnp.float32)
    full = jnp.concatenate([rows.reshape(n, stride, width), marks.reshape(n, stride, goals)], axis=1)
    full = full.astype(jnp.bfloat16)
    send[...] = full[: n - 1]
    recv[n - 1] = full[n - 1]

    pl.semaphore_wait(barrier, n - 1)

    def start(k):
        pltpu.make_async_remote_copy(
            src_ref=send.at[k, pl.ds(0, stride + 2)],
            dst_ref=recv.at[k, pl.ds(0, stride + 2)],
            send_sem=send_sem,
            recv_sem=recv_sem.at[jnp.int32(k >= near)],
            device_id=device(k),
            device_id_type=MESH,
        ).start()

    each(n - 1, start)
    sums = jnp.zeros((goals, width), jnp.float32)
    added = jnp.zeros((stride, goals), jnp.float32)
    for group, lo_slot, hi_slot, count in ((1, near, n, n - 1 - near), (0, 0, near, near)):
        landed = recv.at[pl.ds(lo_slot, count), pl.ds(0, stride + 2)]
        pltpu.make_async_copy(landed, landed, recv_sem.at[group]).wait()
        slots = hi_slot - lo_slot
        data = recv[lo_slot:hi_slot].astype(jnp.float32)
        tags = data[:, stride:]
        s_sub = lax.broadcasted_iota(jnp.int32, (slots, stride, goals), 1)
        s_lane = lax.broadcasted_iota(jnp.int32, (slots, stride, goals), 2)
        spread = jnp.where(s_lane == s_sub + BINS_DEV, jnp.broadcast_to(tags[:, :1], (slots, stride, goals)), 0.0)
        labels = jnp.sum(spread, axis=2, keepdims=True).astype(jnp.int32)
        choose = (s_lane == labels).astype(jnp.float32).reshape(slots * stride, goals).astype(jnp.bfloat16)
        values = data[:, :stride].reshape(slots * stride, width).astype(jnp.bfloat16)
        sums = sums + lax.dot_general(choose, values, (((0,), (0,)), ((), ())), preferred_element_type=jnp.float32)
        added = added + jnp.sum(tags, axis=0)
    low, high = added[:1], added[1:2]
    mass = high + pltpu.roll(high, goals - BINS_DEV, 1) + low
    total = jnp.sum(
        jnp.where((t_lane >= BINS_DEV + stride) & (t_lane < BINS_DEV + stride + 3), low, 0.0), axis=1, keepdims=True
    )
    mass_col = jnp.broadcast_to(mass, (goals, goals)).T
    mean_ref[...] = sums[:BINS_DEV] / (mass_col[:BINS_DEV, :width] + 1.0)
    rarity_ref[...] = jnp.log(total / (BINS_DEV * n)) - jnp.log(mass[:, :BINS_DEV] + 1.0)
    sent = send.at[:, pl.ds(0, stride + 2)]
    pltpu.make_async_copy(sent, sent, send_sem).wait()


def put(mean, rarity, mean_hbm, rarity_hbm, sem):
    copies = [pltpu.make_async_copy(mean, mean_hbm, sem.at[0]), pltpu.make_async_copy(rarity, rarity_hbm, sem.at[1])]
    for c in copies:
        c.start()
    for c in copies:
        c.wait()


def shards(goal_embed, goal_bins, goal_weights):
    goals, width = goal_embed.shape
    across = lax.axis_size("gx")
    along = lax.axis_size("gy")
    n = across * along
    capacity = max(2, 2 * goals // n)
    stride = -(-capacity // 8) * 8
    mean, rarity = pl.pallas_call(
        functools.partial(kernel, across, along, stride),
        out_shape=(
            pltpu.VMEM((BINS_DEV, width), jnp.float32),
            pltpu.VMEM((1, BINS_DEV), jnp.float32),
        ),
        in_specs=[pl.BlockSpec(memory_space=pl.ANY)] * 3,
        out_specs=(pl.BlockSpec(memory_space=pltpu.VMEM),) * 2,
        scratch_shapes=[
            pltpu.VMEM((n - 1, 2 * stride, width), jnp.bfloat16),
            pltpu.VMEM((n, 2 * stride, width), jnp.bfloat16),
            pltpu.SemaphoreType.DMA,
            pltpu.SemaphoreType.DMA((2,)),
            pltpu.VMEM((goals, width), jnp.bfloat16),
            pltpu.VMEM((1, goals), jnp.int32),
            pltpu.VMEM((1, goals), jnp.float32),
            pltpu.SemaphoreType.DMA((3,)),
        ],
        compiler_params=pltpu.CompilerParams(collective_id=0, has_side_effects=True),
    )(goal_embed, goal_bins.reshape(1, goals), goal_weights.reshape(1, goals))
    mean, rarity = pl.pallas_call(
        put,
        out_shape=(
            jax.ShapeDtypeStruct((BINS_DEV, width), jnp.float32),
            jax.ShapeDtypeStruct((1, BINS_DEV), jnp.float32),
        ),
        in_specs=[pl.BlockSpec(memory_space=pltpu.VMEM)] * 2,
        out_specs=(pl.BlockSpec(memory_space=pl.ANY),) * 2,
        scratch_shapes=[pltpu.SemaphoreType.DMA((2,))],
    )(pltpu.with_memory_space_constraint(mean, pltpu.VMEM), pltpu.with_memory_space_constraint(rarity, pltpu.VMEM))
    return mean, rarity.reshape(BINS_DEV)


def solution(mesh):
    in_specs = (P(("gx", "gy"), None), P(("gx", "gy")), P(("gx", "gy")))
    out_specs = (P(("gx", "gy"), None), P(("gx", "gy")))
    return jax.shard_map(shards, mesh=mesh, in_specs=in_specs, out_specs=out_specs, check_vma=False)
```
